128 devices in a mesh: row: 16 (over z_hi, y, core), col: 8 (over x, z_lo).
Axes of the slice: x: 4, y: 4, z: 4 (z_hi: 2, z_lo: 2; z = z_hi * 2 + z_lo), core: 2. Of those that a mesh axis runs over, the one named last changes fastest.
Arguments:
- tokens: bfloat16 [16384, 2048], P(('row', 'col')), may hold values from -30 to 30
- ln1_gain: float32 [2048], replicated, may hold values from 0.25 to 1.75
- qkv_weight: bfloat16 [2048, 16, 3, 128], P('row', 'col'), may hold values from -4 to 4
- out_weight: bfloat16 [2048, 2048], P('col', 'row'), may hold values from -0.125 to 0.125
- ln2_gain: float32 [2048], replicated, may hold values from 0.25 to 1.75
- ffn_in: bfloat16 [2048, 8192], P('row', 'col'), may hold values from -0.125 to 0.125
- ffn_out: bfloat16 [8192, 2048], P('col', 'row'), may hold values from -0.0625 to 0.0625
- expert_ids: int32 [16384, 1], P(('row', 'col')), may hold values from 0 to 63; in each aligned block of 128 rows (0 to 127, 128 to 255, ...) at most 4 rows name the same one
- expert_in: bfloat16 [128, 2048, 2048], P(('row', 'col')), may hold values from -0.125 to 0.125
- expert_out: bfloat16 [128, 2048, 2048], P(('row', 'col')), may hold values from -0.09375 to 0.09375
Outputs:
- block_out: bfloat16 [16384, 2048], P(('row', 'col'))
The draws below stay inside these ranges and needn't reach their ends.
Inputs may be any that keep to these rules, and one draw needn't show every extreme that they name: `expert_ids`: among the tokens of one device no expert is named more than 4 times, and in every draw some expert is named exactly 4 times by the tokens of some device.
All inputs are finite; a program needn't handle non-finite values.
Results may differ from the reference program's by a relative error of at most 0.013.
Values may be sent and summed in bfloat16 or wider, within the bound.
No kernel may reach another device: no remote copies, remote signals or barrier semaphores. Data moves between devices by JAX's collectives and lax.ppermute only.
A program may use at most 128 MiB of HBM per device.

```python
import math
import jax
import jax.numpy as jnp
import numpy as np
from jax import lax

D = 2048
HEADS = 16
DH = 128
FF = 8192
FFE = 4096
TOK_DEV = 128
SEQ = 1024
TOKENS = 16384
EXPERTS = 64
CAP = 4
FF_BLOCK = 1024
HALF = 2048
N_ROW = 16
N_COL = 8


def draw_tokens(key, part):
    first_key = jax.random.fold_in(jax.random.fold_in(key, 11), 0)
    base_values = jax.random.normal(first_key, (TOKENS, D), jnp.float32)
    return jnp.clip(base_values, -30.0, 30.0).astype(jnp.bfloat16)


def draw_qkv_weight(key, part):
    first_key = jax.random.fold_in(jax.random.fold_in(key, 23), 0)
    base_values = jax.random.normal(first_key, (D, HEADS, 3, DH), jnp.float32) * D ** (-0.5)
    factors = jnp.array([2.0, 1.0, 1.0], jnp.float32)[None, None, :, None]
    base_values = base_values * factors
    return jnp.clip(base_values, -4.0, 4.0).astype(jnp.bfloat16)


def block_scale(key, dims, shards, low, high):
    gain, own = 1.0, jax.random.fold_in(key, 6)
    for dim, blocks in shards:
        draws = jnp.exp(jax.random.uniform(jax.random.fold_in(own, dim), (blocks,), jnp.float32, low / len(shards), high / len(shards)))
        gain = gain * jnp.repeat(draws, dims[dim] // blocks).reshape([-1 if axis == dim else 1 for axis in range(len(dims))])
    return gain


def assign_block(key, own, number, rows, count, top, reach, slope):
    ranking = jax.random.permutation(key, count)
    crowded, common = portions_of(count, rows * top, reach, slope, True), portions_of(count, rows * top, reach, slope, False)
    places = jnp.arange(count)

    def named(lengths, offset_by):
        used = int((lengths > 0).sum())
        fixed = max(1, used // 4)
        passed = fixed + (places - fixed + offset_by * (used - fixed)) % max(1, count - fixed)
        return jnp.zeros((count,), jnp.int32).at[ranking[jnp.where(places < fixed, places, passed)]].set(jnp.asarray(lengths, jnp.int32))

    lengths = jnp.where(number % 4 == 0, named(crowded, number // 4), named(common, number - number // 4 - 1))
    mixed = jax.random.permutation(jax.random.fold_in(own, 3), count)
    giver, receiver = mixed[0:count // 2 * 2:2], mixed[1:count // 2 * 2:2]
    margin = jnp.minimum(lengths[giver] - 1, reach - lengths[receiver]) // 2
    margin = jnp.where((giver == ranking[0]) | (receiver == ranking[0]) | (lengths[receiver] == 0), 0, jnp.maximum(margin, 0))
    passed = jax.random.randint(jax.random.fold_in(own, 4), (count // 2,), 0, 1 << 20) % (margin + 1)
    lengths = lengths.at[giver].add(-passed).at[receiver].add(passed)
    members = jnp.searchsorted(jnp.cumsum(lengths), jnp.arange(rows * top), side="right").astype(jnp.int32)
    grid = members.reshape(top, rows).T
    grid = grid[jax.random.permutation(jax.random.fold_in(own, 1), rows)]
    offset_by = jax.random.randint(jax.random.fold_in(own, 2), (rows, 1), 0, top)
    return jnp.take_along_axis(grid, (jnp.arange(top)[None, :] + offset_by) % top, axis=1)


def portions_of(count, total, limit, skew, full):
    weights = [(1 << 20) // math.isqrt(rank ** skew) + 1 for rank in range(1, count + 1)]
    largest = limit if full else min(limit, max(-(-total // count), total * weights[0] // sum(weights)))
    least = 1 if total - largest >= count - 1 else 0
    holding, rest = [largest] + [least] * (count - 1), total - largest - least * (count - 1)
    while rest > 0:
        candidates = [i for i in range(1, count) if holding[i] < largest] or [i for i in range(1, count) if holding[i] < limit]
        whole, remaining = sum([weights[i] for i in candidates]), rest
        for i in candidates:
            extra = min(limit - holding[i], max(1, remaining * weights[i] // whole), rest)
            holding[i] = holding[i] + extra
            rest = rest - extra
    return np.array(holding)


def normal_values(own_key, dims, width, bound, pieces=(), held_as=jnp.bfloat16):
    factor_of = block_scale(own_key, dims, pieces, -0.22, 0.18) if pieces else 1.0
    values = jax.random.normal(own_key, dims, jnp.float32) * width * factor_of
    return jnp.minimum(jnp.maximum(values, -bound), bound).astype(held_as)


def setup_inputs(seed: int = 0) -> dict:
    key_list = jax.random.split(jax.random.key(seed), 11)
    tokens = draw_tokens(jax.random.fold_in(key_list[10], 71), 0)
    ln1_gain = jnp.clip(1.0 + 0.15 * jax.random.normal(key_list[1], (D,), jnp.float32), 0.25, 1.75)
    qkv_weight = draw_qkv_weight(jax.random.fold_in(key_list[10], 71), 0)
    out_weight = normal_values(key_list[3], (HEADS * DH, D), (HEADS * DH) ** -0.5, 0.125, ((0, 8), (1, 16)))
    ln2_gain = jnp.clip(1.0 + 0.15 * jax.random.normal(key_list[4], (D,), jnp.float32), 0.25, 1.75)
    ffn_in = normal_values(key_list[5], (D, FF), D ** -0.5, 0.125, ((0, 16), (1, 8)))
    ffn_out = normal_values(key_list[6], (FF, D), FF ** -0.5, 0.0625, ((0, 8), (1, 16)))
    expert_ids_keys = jax.random.split(jax.random.fold_in(key_list[7], 1), TOKENS // TOK_DEV)
    expert_ids_turns = jax.random.permutation(jax.random.fold_in(key_list[7], 3), TOKENS // TOK_DEV)
    expert_ids = jax.vmap(lambda own, number: assign_block(jax.random.fold_in(key_list[7], 2), own, number, TOK_DEV, EXPERTS, 1, CAP, 2))(expert_ids_keys, expert_ids_turns).reshape((TOKENS, 1))
    expert_in = normal_values(key_list[8], (EXPERTS * 2, D, HALF), D ** -0.5, 0.125, ((0, 128),))
    expert_out = normal_values(key_list[9], (EXPERTS * 2, HALF, D), FFE ** -0.5, 0.09375, ((0, 128),))
    return {"tokens": tokens, "ln1_gain": ln1_gain, "qkv_weight": qkv_weight, "out_weight": out_weight, "ln2_gain": ln2_gain, "ffn_in": ffn_in, "ffn_out": ffn_out, "expert_ids": expert_ids, "expert_in": expert_in, "expert_out": expert_out}


def layer_norm(row_data, gain_vector):
    row_data = row_data.astype(jnp.float32)
    centered = row_data - lax.optimization_barrier(jnp.mean(row_data, axis=-1, keepdims=True))
    spread = lax.optimization_barrier(jnp.mean(centered * centered, axis=-1, keepdims=True))
    return centered * lax.rsqrt(spread + 1e-06) * gain_vector

def attend_head(queries, key_rows, value_rows):
    scores = jnp.dot(queries, key_rows.T, preferred_element_type=jnp.float32) * DH ** (-0.5)
    row_max = lax.optimization_barrier(jnp.max(scores, axis=-1, keepdims=True))
    weights = jnp.exp(scores - row_max)
    probabilities = (weights / lax.optimization_barrier(jnp.sum(weights, axis=-1, keepdims=True))).astype(jnp.bfloat16)
    return jnp.dot(probabilities, value_rows, preferred_element_type=jnp.float32).astype(jnp.bfloat16)

def image_block(image_rows, ln1_gain, qkv_weight, out_weight, ln2_gain, ffn_in, ffn_out):
    normed = layer_norm(image_rows, ln1_gain).astype(jnp.bfloat16)
    projected = jnp.dot(normed, qkv_weight.reshape(D, HEADS * 3 * DH), preferred_element_type=jnp.float32)
    projected = projected.astype(jnp.bfloat16).reshape(SEQ, HEADS, 3, DH)
    by_head = jnp.transpose(projected, (1, 2, 0, 3))
    attended = lax.map(lambda head_item: attend_head(head_item[0], head_item[1], head_item[2]), by_head)
    attended = jnp.transpose(attended, (1, 0, 2)).reshape(SEQ, HEADS * DH)
    mixed_heads = jnp.dot(attended, out_weight, preferred_element_type=jnp.float32)
    hidden_state = (image_rows.astype(jnp.float32) + mixed_heads).astype(jnp.bfloat16)
    normed_two = layer_norm(hidden_state, ln2_gain).astype(jnp.bfloat16)
    inner_sum = jnp.dot(normed_two, ffn_in, preferred_element_type=jnp.float32)
    hidden_units = jax.nn.gelu(inner_sum, approximate=False).astype(jnp.bfloat16)
    dense_sum = jnp.zeros((SEQ, D), jnp.float32)
    for column_block in range(N_COL):
        lower_edge = column_block * FF_BLOCK
        part_sum = jnp.dot(hidden_units[:, lower_edge:lower_edge + FF_BLOCK], ffn_out[lower_edge:lower_edge + FF_BLOCK], preferred_element_type=jnp.float32)
        rounded = lax.optimization_barrier(part_sum.astype(jnp.bfloat16))
        dense_sum = dense_sum + rounded.astype(jnp.float32)
    return (hidden_state, normed_two, dense_sum)

def reference(tokens, ln1_gain, qkv_weight, out_weight, ln2_gain, ffn_in, ffn_out, expert_ids, expert_in, expert_out):
    device_count = N_ROW * N_COL
    images = tokens.reshape(TOKENS // SEQ, SEQ, D)

    def one_image(image_rows):
        return image_block(image_rows, ln1_gain, qkv_weight, out_weight, ln2_gain, ffn_in, ffn_out)
    hidden_state, normed_two, dense_sum = lax.map(one_image, images)
    hidden_state = hidden_state.reshape(TOKENS, D)
    normed_two = normed_two.reshape(TOKENS, D)
    dense_sum = dense_sum.reshape(TOKENS, D)
    chosen = expert_ids[:, 0].astype(jnp.int32)
    by_device = chosen.reshape(device_count, TOK_DEV)
    one_hot = (by_device[:, :, None] == jnp.arange(EXPERTS, dtype=jnp.int32)[None, None, :]).astype(jnp.int32)
    earlier = jnp.cumsum(one_hot, axis=1) - one_hot
    local_slot = lax.optimization_barrier(jnp.sum(earlier * one_hot, axis=2))
    global_slot = (local_slot + CAP * jnp.arange(device_count, dtype=jnp.int32)[:, None]).reshape(TOKENS).astype(jnp.int32)
    buffers = jnp.zeros((EXPERTS, device_count * CAP, D), normed_two.dtype).at[chosen, global_slot].set(normed_two)
    paired_in = expert_in.reshape(EXPERTS, 2, D, HALF)
    paired_out = expert_out.reshape(EXPERTS, 2, HALF, D)

    def run_expert(operands):
        buffer_rows, weights_in, weights_out = operands
        whole_in = jnp.concatenate((weights_in[0], weights_in[1]), axis=1)
        whole_out = jnp.concatenate((weights_out[0], weights_out[1]), axis=0)
        inner_units = jax.nn.gelu(jnp.dot(buffer_rows, whole_in, preferred_element_type=jnp.float32), approximate=False).astype(jnp.bfloat16)
        return jnp.dot(inner_units, whole_out, preferred_element_type=jnp.float32).astype(jnp.bfloat16)
    results = lax.map(run_expert, (buffers, paired_in, paired_out))
    expert_rows = results[chosen, global_slot]
    block_out = hidden_state.astype(jnp.float32) + dense_sum + expert_rows.astype(jnp.float32)
    return block_out.astype(jnp.bfloat16)
```

```python
import functools

import jax
import jax.numpy as jnp
from jax import lax
from jax.experimental import pallas as pl
from jax.experimental.pallas import tpu as pltpu
from jax.sharding import Mesh
from jax.sharding import PartitionSpec as P

ALL = ("zh", "y", "c", "x", "zl")
Z = ("zh", "zl")
BF16 = jnp.bfloat16
F32 = jnp.float32
VMEM_LIMIT = 60 * 2**20


def gelu(value):
    return value * 0.5 * (1.0 + lax.erf(value * (0.5**0.5)))


def moved(array, axis, step):
    return lax.ppermute(array, axis, [(i, (i + step) % 4) for i in range(4)])


def swapped(array, axis):
    return lax.ppermute(array, axis, [(0, 1), (1, 0)])


def ring_parts(array, axis):
    half = array.shape[0] // 2
    back, ahead = moved(array, axis, 1), moved(array, axis, 3)
    far_low, far_high = moved(back[:half], axis, 1), moved(ahead[half:], axis, 3)
    return array, back, ahead, far_low, far_high


def ring_stack(array, axis):
    own, back, ahead, far_low, far_high = ring_parts(array, axis)
    return jnp.stack([own, back, ahead, jnp.concatenate([far_low, far_high])])


def ring_slot(index, own):
    away = lax.rem(index - own + 4, 4)
    return jnp.where(away == 0, 0, jnp.where(away == 3, 1, jnp.where(away == 1, 2, 3)))


def layer_norm(rows, gain):
    rows = rows.astype(F32)
    centered = rows - jnp.mean(rows, axis=-1, keepdims=True)
    spread = jnp.mean(centered * centered, axis=-1, keepdims=True)
    return centered * lax.rsqrt(spread + 1e-06) * gain


def pairs_swapped(rows, flag):
    count, width = rows.shape
    paired = rows.reshape(count, width // 256, 2, 128)
    return jnp.where(flag == 0, paired, paired[:, :, ::-1]).reshape(count, width)


def qkv_attention_kernel(pos, x_ref, own_ref, other_ref, o_ref, weight, projected):
    for zh in range(2):
        for y in range(4):
            at = (zh * 4 + y) * 256
            weight[at : at + 128] = own_ref[pos[y], pos[8 + zh]]
            weight[at + 128 : at + 256] = other_ref[pos[y], pos[8 + zh]]

    @pl.loop(0, 4)
    def _(i):
        rows = pl.ds(pl.multiple_of(i * 256, 256), 256)
        projected[rows] = jnp.dot(x_ref[rows], weight[...], preferred_element_type=F32).astype(BF16)

    @pl.loop(0, 8)
    def _(i):
        rows = pl.ds(pl.multiple_of(i * 128, 128), 128)
        outs = []
        for head in range(2):
            at = head * 128
            query = projected[rows, at : at + 128]
            key = projected[:, 256 + at : 384 + at]
            value = projected[:, 512 + at : 640 + at]
            scores = lax.dot_general(query, key, (((1,), (1,)), ((), ())), preferred_element_type=F32)
            scores = scores * (128**-0.5)
            weights = jnp.exp(scores - jnp.max(scores, axis=-1, keepdims=True))
            total = jnp.sum(weights, axis=-1, keepdims=True)
            probabilities = (weights / total).astype(BF16)
            outs.append(jnp.dot(probabilities, value, preferred_element_type=F32).astype(BF16))
        o_ref[pos[10 + i]] = jnp.concatenate(outs, axis=1)


def qkv_attention(pos, rows, own, other):
    return pl.pallas_call(
        qkv_attention_kernel,
        grid_spec=pltpu.PrefetchScalarGridSpec(
            num_scalar_prefetch=1,
            grid=(1,),
            in_specs=[
                pl.BlockSpec((1024, 2048), lambda i, p: (0, 0)),
                pl.BlockSpec((4, 2, 128, 768), lambda i, p: (0, 0, 0, 0)),
                pl.BlockSpec((4, 2, 128, 768), lambda i, p: (0, 0, 0, 0)),
            ],
            out_specs=pl.BlockSpec((8, 128, 256), lambda i, p: (0, 0, 0)),
            scratch_shapes=[pltpu.VMEM((2048, 768), BF16), pltpu.VMEM((1024, 768), BF16)],
        ),
        out_shape=jax.ShapeDtypeStruct((8, 128, 256), BF16),
        compiler_params=pltpu.CompilerParams(vmem_limit_bytes=VMEM_LIMIT),
        cost_estimate=pl.CostEstimate(flops=6 * 10**9, bytes_accessed=8 * 2**20, transcendentals=2**21),
        name="qkv_attention",
    )(pos, rows, own, other)


def out_kernel(pos, a_ref, own_ref, other_ref, t_ref, g_ref, hidden_ref, normed_ref, product):
    step = pl.program_id(0)
    heads = jnp.concatenate([a_ref[i] for i in range(8)], axis=1)
    y = pos[18 + step]
    for zh in range(2):
        for side, ref in ((0, own_ref), (1, other_ref)):
            block = jnp.concatenate(
                [ref[pos[22 + x], 0, pos[4 + 2 * zh + zl]] for x in range(4) for zl in range(2)], axis=0
            )
            product[zh * 8 + y * 2 + side] = jnp.dot(heads, block, preferred_element_type=F32)

    @pl.when(step == pl.num_programs(0) - 1)
    def _():
        core = pos[26]
        columns = []
        for pair in range(8):
            first, second = product[2 * pair + core], product[2 * pair + 1 - core]
            columns += [first, second]
        mixed = jnp.concatenate(columns, axis=1)
        hidden = (t_ref[...].astype(F32) + mixed).astype(BF16)
        hidden_ref[...] = hidden
        normed_ref[...] = layer_norm(hidden, g_ref[...]).astype(BF16)


def out_projection(pos, attended, own, other, tokens, gain):
    weights = pl.BlockSpec((4, 1, 4, 256, 128), lambda i, p: (0, i, 0, 0, 0))
    whole = pl.BlockSpec((128, 2048), lambda i, p: (0, 0))
    return pl.pallas_call(
        out_kernel,
        grid_spec=pltpu.PrefetchScalarGridSpec(
            num_scalar_prefetch=1,
            grid=(4,),
            in_specs=[
                pl.BlockSpec((8, 128, 256), lambda i, p: (0, 0, 0)),
                weights,
                weights,
                whole,
                pl.BlockSpec((1, 2048), lambda i, p: (0, 0)),
            ],
            out_specs=[whole, whole],
            scratch_shapes=[pltpu.VMEM((16, 128, 128), F32)],
        ),
        out_shape=[jax.ShapeDtypeStruct((128, 2048), BF16)] * 2,
        compiler_params=pltpu.CompilerParams(vmem_limit_bytes=VMEM_LIMIT),
        cost_estimate=pl.CostEstimate(flops=3 * 10**9, bytes_accessed=9 * 2**20, transcendentals=0),
        name="out_projection",
    )(pos, attended, own, other, tokens, gain)


def accumulate(step, last, part, total, o_ref):
    @pl.when(step == 0)
    def _():
        total[...] = part

    @pl.when((step > 0) & (step < last))
    def _():
        total[...] += part

    @pl.when(step == last)
    def _():
        o_ref[...] = (total[...] + part).astype(BF16).reshape(o_ref.shape)


def dense_kernel(pos, x_ref, ao0, ao1, at0, at1, bo0, bo1, bt0, bt1, o_ref, total):
    step = pl.program_id(0)
    ups = ((ao0, at0), (ao1, at1))
    downs = ((bo0, bt0), (bo1, bt1))
    up = jnp.concatenate([ref[0, pos[y]] for zh in range(2) for y in range(4) for ref in ups[zh]], axis=0)
    inner = gelu(jnp.dot(x_ref[...], up, preferred_element_type=F32)).astype(BF16)
    down = jnp.concatenate([ref[pos[y], 0] for zh in range(2) for y in range(4) for ref in downs[zh]], axis=1)
    part = jnp.dot(inner, down, preferred_element_type=F32)
    accumulate(step, pl.num_programs(0) - 1, part, total, o_ref)


def dense_branch(pos, rows, up_own, up_other, down_own, down_other):
    width = 512

    def up(zh):
        return pl.BlockSpec((1, 4, 128, width), lambda j, p: (p[4 + 2 * zh + j // 2], 0, 0, j % 2))

    def down(zh):
        return pl.BlockSpec((4, 1, width, 128), lambda j, p: (0, p[4 + 2 * zh + j // 2], j % 2, 0))

    whole = pl.BlockSpec((512, 2048), lambda j, p: (0, 0))
    return pl.pallas_call(
        dense_kernel,
        grid_spec=pltpu.PrefetchScalarGridSpec(
            num_scalar_prefetch=1,
            grid=(4,),
            in_specs=[whole, up(0), up(1), up(0), up(1), down(0), down(1), down(0), down(1)],
            out_specs=whole,
            scratch_shapes=[pltpu.VMEM((512, 2048), F32)],
        ),
        out_shape=jax.ShapeDtypeStruct((512, 2048), BF16),
        compiler_params=pltpu.CompilerParams(vmem_limit_bytes=VMEM_LIMIT),
        cost_estimate=pl.CostEstimate(flops=12 * 10**9, bytes_accessed=20 * 2**20, transcendentals=2**20),
        name="dense_branch",
    )(pos, rows, up_own, up_own, up_other, up_other, down_own, down_own, down_other, down_other)


def expert_kernel(x_ref, up_ref, down_ref, o_ref, rows, total):
    step = pl.program_id(0)

    @pl.when(step == 0)
    def _():
        rows[...] = x_ref[...].reshape(512, 2048)

    inner = gelu(jnp.dot(rows[...], up_ref[...], preferred_element_type=F32)).astype(BF16)
    part = jnp.dot(inner, down_ref[...], preferred_element_type=F32)
    accumulate(step, pl.num_programs(0) - 1, part, total, o_ref)


def expert_branch(rows, up, down):
    width = 512
    whole = pl.BlockSpec((128, 4, 2048), lambda j: (0, 0, 0))
    return pl.pallas_call(
        expert_kernel,
        grid=(2048 // width,),
        in_specs=[
            whole,
            pl.BlockSpec((None, 2048, width), lambda j: (0, 0, j)),
            pl.BlockSpec((None, width, 2048), lambda j: (0, j, 0)),
        ],
        out_specs=whole,
        out_shape=jax.ShapeDtypeStruct((128, 4, 2048), BF16),
        scratch_shapes=[pltpu.VMEM((512, 2048), BF16), pltpu.VMEM((512, 2048), F32)],
        compiler_params=pltpu.CompilerParams(vmem_limit_bytes=VMEM_LIMIT),
        cost_estimate=pl.CostEstimate(flops=12 * 10**9, bytes_accessed=20 * 2**20, transcendentals=2**20),
        name="expert_branch",
    )(rows, up, down)


def summed_home(partial):
    own, back, ahead = partial[:128], partial[128:256], partial[256:384]
    low = moved(partial[384:448], "x", 1).astype(F32)
    high = moved(partial[448:], "x", 3).astype(F32)
    back, ahead = back.astype(F32), ahead.astype(F32)
    to_ahead = jnp.concatenate([ahead[:64] + low, ahead[64:]]).astype(BF16)
    to_back = jnp.concatenate([back[:64], back[64:] + high]).astype(BF16)
    from_back, from_ahead = moved(to_ahead, "x", 1), moved(to_back, "x", 3)
    return own.astype(F32) + from_back.astype(F32) + from_ahead.astype(F32)


def shards(tokens, ln1_gain, qkv_weight, out_weight, ln2_gain, ffn_in, ffn_out, expert_ids, expert_in, expert_out):
    zh, y, c, x, zl = (lax.axis_index(name) for name in ALL)
    z = zh * 2 + zl
    four = jnp.arange(4, dtype=jnp.int32)
    rel_rows = []
    for far in range(2):
        for away in (0, 3, 1, 2):
            rel_rows.append(lax.rem(x + away, 4) * 2 + (zl ^ far))
    pos = jnp.concatenate(
        [
            ring_slot(four, y),
            ring_slot(four, z),
            jnp.stack([zh, 1 - zh]),
            jnp.stack(rel_rows),
            jnp.stack([y, lax.rem(y + 3, 4), lax.rem(y + 1, 4), lax.rem(y + 2, 4)]),
            ring_slot(four, x),
            c[None],
        ]
    ).astype(jnp.int32)

    normed = pairs_swapped(layer_norm(tokens, ln1_gain).astype(BF16), c)
    own, back, ahead, far_low, far_high = ring_parts(normed, "x")
    side = swapped(normed, "zl")
    side_back, side_ahead = moved(side, "x", 1), moved(side, "x", 3)
    side_far = [swapped(far_low, "zl"), swapped(far_high, "zl")]
    image = jnp.concatenate([own, back, ahead, far_low, far_high, side, side_back, side_ahead, *side_far])

    qkv = qkv_weight.transpose(0, 2, 1, 3).reshape(128, 768)
    qkv = ring_stack(jnp.stack([qkv, swapped(qkv, "zh")]), "y")
    qkv_other = swapped(qkv, "c")
    out_own = ring_stack(ring_stack(ring_stack(out_weight, Z), "y"), "x")
    out_other = swapped(out_own, "c")
    up_own = ring_stack(ring_stack(ffn_in, "y"), Z)
    up_other = swapped(up_own, "c")
    down_own = ring_stack(ring_stack(ffn_out, Z), "y")
    down_other = swapped(down_own, "c")

    attended = qkv_attention(pos, image, qkv, qkv_other)
    attended = lax.all_to_all(attended, ("x", "zl"), 0, 0, tiled=True)
    hidden, normed_two = out_projection(pos, attended, out_own, out_other, tokens, ln2_gain[None])

    chosen = expert_ids[:, 0]
    expert_range = jnp.arange(64, dtype=jnp.int32)
    one_hot = (chosen[:, None] == expert_range[None, :]).astype(jnp.int32)
    earlier = jnp.cumsum(one_hot, axis=0) - one_hot
    slot = jnp.sum(earlier * one_hot, axis=1)
    position = chosen * 4 + slot
    placing = (jnp.arange(256, dtype=jnp.int32)[:, None] == position[None, :]).astype(BF16)
    table = jnp.dot(placing, normed_two, preferred_element_type=F32).astype(BF16)
    outgoing = jnp.repeat(table.reshape(64, 4, 2048), 2, axis=0)
    arrived = lax.all_to_all(outgoing, ALL, 0, 0, tiled=True)

    gathered = jnp.concatenate(ring_parts(pairs_swapped(normed_two, c), "x"))
    dense = dense_branch(pos, gathered, up_own, up_other, down_own, down_other)
    dense_sum = pairs_swapped(summed_home(dense), c)

    halves = expert_branch(arrived, expert_in, expert_out)
    returned = lax.all_to_all(halves, ALL, 0, 0, tiled=True).reshape(512, 2048)
    place = jnp.arange(512, dtype=jnp.int32)[None, :]
    first = (8 * chosen + slot)[:, None]
    picking = ((place == first) | (place == first + 4)).astype(BF16)
    expert_sum = jnp.dot(picking, returned, preferred_element_type=F32)
    return (hidden.astype(F32) + dense_sum + expert_sum).astype(BF16)


def solution(mesh):
    split = Mesh(mesh.devices.reshape(2, 4, 2, 4, 2), ALL)
    row, col = ("zh", "y", "c"), ("x", "zl")
    in_specs = (
        P(ALL, None),
        P(),
        P(row, col, None, None),
        P(col, row),
        P(),
        P(row, col),
        P(col, row),
        P(ALL, None),
        P(ALL, None, None),
        P(ALL, None, None),
    )
    return jax.shard_map(shards, mesh=split, in_specs=in_specs, out_specs=P(ALL, None), check_vma=False)
```

```python
import jax
import jax.numpy as jnp
from jax import lax
from jax.experimental import pallas as pl
from jax.experimental.pallas import tpu as pltpu
from jax.sharding import Mesh
from jax.sharding import PartitionSpec as P


ALL = ("zh", "y", "c", "x", "zl")
BF16 = jnp.bfloat16
F32 = jnp.float32
VMEM_LIMIT = 60 * 2**20


def gelu(value):
    return value * 0.5 * (1.0 + lax.erf(value * (0.5**0.5)))


def moved(array, axis, step):
    return lax.ppermute(array, axis, [(i, (i + step) % 4) for i in range(4)])


def swapped(array, axis):
    return lax.ppermute(array, axis, [(0, 1), (1, 0)])


def exchanged(array, axes):
    return lax.all_to_all(array, axes, 0, 0, tiled=True)


def copies_of_all(array, axes):
    return exchanged(jnp.broadcast_to(array, (lax.axis_size(axes), *array.shape)), axes)


def ring_parts(array, axis):
    half = array.shape[0] // 2
    back, ahead = moved(array, axis, 1), moved(array, axis, 3)
    far_low, far_high = moved(back[:half], axis, 1), moved(ahead[half:], axis, 3)
    return array, back, ahead, far_low, far_high


def ring_stack(array, axis):
    own, back, ahead, far_low, far_high = ring_parts(array, axis)
    return jnp.stack([own, back, ahead, jnp.concatenate([far_low, far_high])])


def ring_slot(index, own):
    away = lax.rem(index - own + 4, 4)
    return jnp.where(away == 0, 0, jnp.where(away == 3, 1, jnp.where(away == 1, 2, 3)))


def layer_norm(rows, gain):
    rows = rows.astype(F32)
    centered = rows - jnp.mean(rows, axis=-1, keepdims=True)
    spread = jnp.mean(centered * centered, axis=-1, keepdims=True)
    return centered * lax.rsqrt(spread + 1e-06) * gain


def core_block(pos, place):
    pair, side = place // 2, place % 2
    return pl.ds(pl.multiple_of((2 * pair + (side ^ pos[9])) * 128, 128), 128)


def whole_spec(shape):
    return pl.BlockSpec(shape, lambda i, p: (0,) * len(shape))


def norm_kernel(pos, x_ref, g_ref, o_ref, rows):
    rows[...] = layer_norm(x_ref[...], g_ref[...]).astype(BF16)
    for place in range(16):
        o_ref[:, place * 128 : place * 128 + 128] = rows[:, core_block(pos, place)]


def first_norm(pos, tokens, gain):
    return pl.pallas_call(
        norm_kernel,
        grid_spec=pltpu.PrefetchScalarGridSpec(
            num_scalar_prefetch=1,
            grid=(1,),
            in_specs=[whole_spec((128, 2048)), whole_spec((1, 2048))],
            out_specs=whole_spec((128, 2048)),
            scratch_shapes=[pltpu.VMEM((128, 2048), BF16)],
        ),
        out_shape=jax.ShapeDtypeStruct((128, 2048), BF16),
        compiler_params=pltpu.CompilerParams(vmem_limit_bytes=VMEM_LIMIT),
        cost_estimate=pl.CostEstimate(flops=10**9, bytes_accessed=2**20, transcendentals=0),
        name="first_norm",
    )(pos, tokens, gain)


def qkv_attention_kernel(pos, *refs):
    pieces, (own_ref, other_ref, o_ref, weight, projected) = refs[:10], refs[10:]
    for zh in range(2):
        for y in range(4):
            at = (zh * 4 + y) * 256
            weight[at : at + 128] = own_ref[pos[y], zh ^ pos[8]]
            weight[at + 128 : at + 256] = other_ref[pos[y], zh ^ pos[8]]

    for part, group in enumerate(((0, 1), (2, 3, 4), (5, 6), (7, 8, 9))):
        rows = jnp.concatenate([pieces[i][...] for i in group], axis=0)
        projected[part * 256 : part * 256 + 256] = jnp.dot(
            rows, weight[...], preferred_element_type=F32
        ).astype(BF16)

    @pl.loop(0, 4)
    def _(i):
        rows = pl.ds(pl.multiple_of(i * 256, 256), 256)
        outs = []
        for head in range(2):
            at = head * 128
            query = projected[rows, at : at + 128]
            key = projected[:, 256 + at : 384 + at]
            value = projected[:, 512 + at : 640 + at]
            scores = lax.dot_general(query, key, (((1,), (1,)), ((), ())), preferred_element_type=F32)
            top = jnp.max(scores, axis=-1, keepdims=True)
            weights = jnp.exp2((scores - top) * (128**-0.5 * 1.4426950408889634))
            total = jnp.sum(weights, axis=-1, keepdims=True)
            mixed = jnp.dot(weights.astype(BF16), value, preferred_element_type=F32)
            outs.append((mixed / total).astype(BF16))
        both = jnp.concatenate(outs, axis=1)
        o_ref[pos[10 + 2 * i]] = both[:128]
        o_ref[pos[11 + 2 * i]] = both[128:]


def qkv_attention(pos, pieces, own, other):
    return pl.pallas_call(
        qkv_attention_kernel,
        grid_spec=pltpu.PrefetchScalarGridSpec(
            num_scalar_prefetch=1,
            grid=(1,),
            in_specs=[whole_spec(piece.shape) for piece in pieces] + [whole_spec((4, 2, 128, 768))] * 2,
            out_specs=whole_spec((8, 128, 256)),
            scratch_shapes=[pltpu.VMEM((2048, 768), BF16), pltpu.VMEM((1024, 768), BF16)],
        ),
        out_shape=jax.ShapeDtypeStruct((8, 128, 256), BF16),
        compiler_params=pltpu.CompilerParams(vmem_limit_bytes=VMEM_LIMIT),
        cost_estimate=pl.CostEstimate(flops=12 * 10**9, bytes_accessed=8 * 2**20, transcendentals=2**21),
        name="qkv_attention",
    )(pos, *pieces, own, other)


def out_kernel(pos, a_ref, *refs):
    own, other = refs[:5], refs[5:10]
    t_ref, g_ref, p_ref, hidden_ref, normed_ref, table_ref, product = refs[10:]
    step = pl.program_id(0)
    heads = jnp.concatenate([a_ref[2 * pos[4 + r] + zl] for r in range(4) for zl in range(2)], axis=1)
    for zh in range(2):
        sides = []
        for held in (own, other):
            blocks = [held[r][2 * zh + zl, 0] for r in range(3) for zl in range(2)]
            blocks += [held[3 + zh][zl, 0] for zl in range(2)]
            sides.append(jnp.concatenate(blocks, axis=0))
        both = jnp.dot(heads, jnp.concatenate(sides, axis=1), preferred_element_type=F32)
        product[zh * 8 + step * 2 + pos[9]] = both[:, :128]
        product[zh * 8 + step * 2 + 1 - pos[9]] = both[:, 128:]

    @pl.when(step == pl.num_programs(0) - 1)
    def _():
        mixed = jnp.concatenate([product[i] for i in range(16)], axis=1)
        hidden = (t_ref[...].astype(F32) + mixed).astype(BF16)
        hidden_ref[...] = hidden
        normed = layer_norm(hidden, g_ref[...]).astype(BF16)
        normed_ref[...] = normed
        slots = lax.broadcasted_iota(jnp.int32, (256, 128), 0)
        placing = jnp.where(slots == p_ref[...], 1.0, 0.0).astype(BF16)
        table = jnp.dot(placing, normed, preferred_element_type=F32).astype(BF16).reshape(64, 4, 2048)
        table_ref[:, 0] = table
        table_ref[:, 1] = table


def out_projection(pos, attended, own, other, tokens, gain, position):
    whole = whole_spec((128, 2048))
    weights = [
        pl.BlockSpec((piece.shape[0], 1, 256, 128), lambda i, p: (0, i, 0, 0)) for piece in (*own, *other)
    ]
    return pl.pallas_call(
        out_kernel,
        grid_spec=pltpu.PrefetchScalarGridSpec(
            num_scalar_prefetch=1,
            grid=(4,),
            in_specs=[
                whole_spec((8, 128, 256)),
                *weights,
                whole,
                whole_spec((1, 2048)),
                whole_spec((1, 128)),
            ],
            out_specs=[whole, whole, whole_spec((64, 2, 4, 2048))],
            scratch_shapes=[pltpu.VMEM((16, 128, 128), F32)],
        ),
        out_shape=[jax.ShapeDtypeStruct((128, 2048), BF16)] * 2 + [jax.ShapeDtypeStruct((64, 2, 4, 2048), BF16)],
        compiler_params=pltpu.CompilerParams(vmem_limit_bytes=VMEM_LIMIT),
        cost_estimate=pl.CostEstimate(flops=6 * 10**9, bytes_accessed=9 * 2**20, transcendentals=0),
        name="out_projection",
    )(pos, attended, *own, *other, tokens, gain, position)


def accumulate(step, last, part, total, write):
    @pl.when(step == 0)
    def _():
        total[...] = part

    @pl.when((step > 0) & (step < last))
    def _():
        total[...] += part

    @pl.when(step == last)
    def _():
        write((total[...] + part).astype(BF16))


def dense_kernel(*refs):
    pieces, (up_ref, down_ref) = refs[:2], refs[2:4]
    outs, (rows, total) = refs[4:6], refs[6:]
    step = pl.program_id(0)

    @pl.when(step == 0)
    def _():
        for i, piece in enumerate(pieces):
            rows[128 * i : 128 * i + 128] = piece[...]

    width = up_ref.shape[-1]
    up = up_ref[...].reshape(2048, width)
    inner = gelu(jnp.dot(rows[...], up, preferred_element_type=F32)).astype(BF16)
    down = jnp.concatenate(
        [
            jnp.concatenate([down_ref[0, r, :, at : at + 128] for r in range(16)], axis=1)
            for at in range(0, width, 128)
        ],
        axis=0,
    )
    part = jnp.dot(inner, down, preferred_element_type=F32)

    def write(value):
        for i, out in enumerate(outs):
            out[...] = value[128 * i : 128 * i + 128]

    accumulate(step, pl.num_programs(0) - 1, part, total, write)


def dense_branch(pieces, weights):
    width = 512
    whole = [pl.BlockSpec(piece.shape, lambda j: (0, 0)) for piece in pieces]
    up = pl.BlockSpec((1, 16, 128, width), lambda j: (j // 2, 0, 0, j % 2))
    down = pl.BlockSpec((1, 16, 128, width), lambda j: (j // 2, 0, 1, j % 2))
    return pl.pallas_call(
        dense_kernel,
        grid=(4,),
        in_specs=whole + [up, down],
        out_specs=whole,
        scratch_shapes=[pltpu.VMEM((256, 2048), BF16), pltpu.VMEM((256, 2048), F32)],
        out_shape=[jax.ShapeDtypeStruct(piece.shape, BF16) for piece in pieces],
        compiler_params=pltpu.CompilerParams(vmem_limit_bytes=VMEM_LIMIT),
        cost_estimate=pl.CostEstimate(flops=7 * 10**9, bytes_accessed=20 * 2**20, transcendentals=2**20),
        name="dense_branch",
    )(*pieces, weights, weights)


def expert_kernel(x_ref, up_ref, down_ref, o_ref, rows, total):
    step = pl.program_id(0)

    @pl.when(step == 0)
    def _():
        rows[...] = x_ref[...].reshape(512, 2048)

    inner = gelu(jnp.dot(rows[...], up_ref[...], preferred_element_type=F32)).astype(BF16)
    part = jnp.dot(inner, down_ref[...], preferred_element_type=F32)

    def write(value):
        o_ref[...] = value.reshape(128, 4, 2048)

    accumulate(step, pl.num_programs(0) - 1, part, total, write)


def expert_branch(rows, up, down):
    width = 512
    whole = pl.BlockSpec((128, 4, 2048), lambda j: (0, 0, 0))
    return pl.pallas_call(
        expert_kernel,
        grid=(2048 // width,),
        in_specs=[
            whole,
            pl.BlockSpec((None, 2048, width), lambda j: (0, 0, j)),
            pl.BlockSpec((None, width, 2048), lambda j: (0, j, 0)),
        ],
        out_specs=whole,
        out_shape=jax.ShapeDtypeStruct((128, 4, 2048), BF16),
        scratch_shapes=[pltpu.VMEM((512, 2048), BF16), pltpu.VMEM((512, 2048), F32)],
        compiler_params=pltpu.CompilerParams(vmem_limit_bytes=VMEM_LIMIT),
        cost_estimate=pl.CostEstimate(flops=12 * 10**9, bytes_accessed=20 * 2**20, transcendentals=2**20),
        name="expert_branch",
    )(rows, up, down)


def final_kernel(h_ref, own_ref, back_ref, ahead_ref, far_ref, r_ref, s_ref, o_ref):
    place = lax.broadcasted_iota(jnp.int32, (128, 512), 1)
    first = s_ref[...]
    picking = jnp.where((place == first) | (place == first + 4), 1.0, 0.0).astype(BF16)
    experts = jnp.dot(picking, r_ref[...].reshape(512, 2048), preferred_element_type=F32)
    dense = own_ref[...].astype(F32) + back_ref[...].astype(F32)
    dense += ahead_ref[...].astype(F32) + far_ref[...].astype(F32)
    o_ref[...] = (h_ref[...].astype(F32) + dense + experts).astype(BF16)


def combined(hidden, dense, returned, first):
    return pl.pallas_call(
        final_kernel,
        out_shape=jax.ShapeDtypeStruct((128, 2048), BF16),
        compiler_params=pltpu.CompilerParams(vmem_limit_bytes=VMEM_LIMIT),
        cost_estimate=pl.CostEstimate(flops=10**9, bytes_accessed=4 * 2**20, transcendentals=0),
        name="combined",
    )(hidden, *dense, returned, first)


def shards(tokens, ln1_gain, qkv_weight, out_weight, ln2_gain, ffn_in, ffn_out, expert_ids, expert_in, expert_out):
    zh, y, c, x, zl = (lax.axis_index(name) for name in ALL)
    ring = [x, lax.rem(x + 3, 4), lax.rem(x + 1, 4), lax.rem(x + 2, 4)]
    rel_rows = [place * 2 + (zl ^ far) for far in range(2) for place in ring]
    pos = jnp.concatenate(
        [ring_slot(jnp.arange(4, dtype=jnp.int32), y), jnp.stack([*ring, zh, c, *rel_rows])]
    ).astype(jnp.int32)

    chosen = expert_ids[:, 0]
    expert_range = jnp.arange(64, dtype=jnp.int32)
    one_hot = (chosen[:, None] == expert_range[None, :]).astype(jnp.int32)
    earlier = jnp.cumsum(one_hot, axis=0) - one_hot
    slot = jnp.sum(earlier * one_hot, axis=1)
    position = (chosen * 4 + slot)[None, :]
    first = (8 * chosen + slot)[:, None]

    down_blocks = ffn_out.reshape(8, 128, 128).transpose(1, 0, 2).reshape(128, 1024)
    packed = jnp.concatenate([ffn_in, down_blocks])
    dense_weights = lax.all_gather(packed, ("zl", "zh", "y", "c")).reshape(2, 16, 256, 1024)

    out_block = copies_of_all(out_weight, ("zh", "zl", "y")).reshape(4, 4, 256, 128)
    normed = first_norm(pos, tokens, ln1_gain[None])
    qkv = qkv_weight.transpose(0, 2, 1, 3).reshape(128, 768)
    qkv = ring_stack(jnp.stack([qkv, swapped(qkv, "zh")]), "y")
    own, back, ahead, far_low, far_high = ring_parts(normed, "x")
    side = swapped(normed, "zl")
    side_back, side_ahead = moved(side, "x", 1), moved(side, "x", 3)
    side_low, side_high = swapped(far_low, "zl"), swapped(far_high, "zl")
    image = [own, back, ahead, far_low, far_high, side, side_back, side_ahead, side_low, side_high]
    qkv_other = swapped(qkv, "c")

    out_own = ring_parts(out_block, "x")
    out_other = [swapped(piece, "c") for piece in out_own]

    attended = qkv_attention(pos, image, qkv, qkv_other)
    attended = exchanged(attended, ("x", "zl"))
    hidden, normed_two, outgoing = out_projection(pos, attended, out_own, out_other, tokens, ln2_gain[None], position)

    arrived = exchanged(outgoing.reshape(128, 4, 2048), ALL)
    from_back, from_ahead, from_far = (
        moved(normed_two, "x", step) for step in (1, 3, 2)
    )
    halves = expert_branch(arrived, expert_in, expert_out)
    returned = exchanged(halves, ALL)

    to_far, to_ahead = dense_branch((from_far, from_ahead), dense_weights)
    to_back, dense = dense_branch((from_back, normed_two), dense_weights)
    home = [moved(to_far, "x", 2), moved(to_ahead, "x", 1), moved(to_back, "x", 3)]
    return combined(hidden, [dense, *home], returned, first)


def solution(mesh):
    split = Mesh(mesh.devices.reshape(2, 4, 2, 4, 2), ALL)
    row, col = ("zh", "y", "c"), ("x", "zl")
    in_specs = (
        P(ALL, None),
        P(),
        P(row, col, None, None),
        P(col, row),
        P(),
        P(row, col),
        P(col, row),
        P(ALL, None),
        P(ALL, None, None),
        P(ALL, None, None),
    )

    return jax.shard_map(shards, mesh=split, in_specs=in_specs, out_specs=P(ALL, None), check_vma=False)
```

```python
import jax
import jax.numpy as jnp
from jax import lax
from jax.experimental import pallas as pl
from jax.experimental.pallas import tpu as pltpu
from jax.sharding import Mesh
from jax.sharding import PartitionSpec as P


ALL = ("zh", "y", "c", "x", "zl")
BF16 = jnp.bfloat16
F32 = jnp.float32
VMEM_LIMIT = 60 * 2**20


def gelu(value):
    return value * 0.5 * (1.0 + lax.erf(value * (0.5**0.5)))


def moved(array, axis, step):
    return lax.ppermute(array, axis, [(i, (i + step) % 4) for i in range(4)])


def swapped(array, axis):
    return lax.ppermute(array, axis, [(0, 1), (1, 0)])


def exchanged(array, axes):
    return lax.all_to_all(array, axes, 0, 0, tiled=True)


def copies_of_all(array, axes):
    return exchanged(jnp.broadcast_to(array, (lax.axis_size(axes), *array.shape)), axes)


def ring_parts(array, axis):
    half = array.shape[0] // 2
    back, ahead = moved(array, axis, 1), moved(array, axis, 3)
    far_low, far_high = moved(back[:half], axis, 1), moved(ahead[half:], axis, 3)
    return array, back, ahead, far_low, far_high


def ring_slot(index, own):
    away = lax.rem(index - own + 4, 4)
    return jnp.where(away == 0, 0, jnp.where(away == 3, 1, jnp.where(away == 1, 2, 3)))


def layer_norm(rows, gain):
    rows = rows.astype(F32)
    centered = rows - jnp.mean(rows, axis=-1, keepdims=True)
    spread = jnp.mean(centered * centered, axis=-1, keepdims=True)
    return centered * lax.rsqrt(spread + 1e-06) * gain


def core_block(pos, place):
    pair, side = place // 2, place % 2
    return pl.ds(pl.multiple_of((2 * pair + (side ^ pos[9])) * 128, 128), 128)


def whole_spec(shape):
    return pl.BlockSpec(shape, lambda i, p: (0,) * len(shape))


def norm_kernel(pos, x_ref, g_ref, o_ref, rows):
    rows[...] = layer_norm(x_ref[...], g_ref[...]).astype(BF16)
    for place in range(16):
        o_ref[:, place * 128 : place * 128 + 128] = rows[:, core_block(pos, place)]


def first_norm(pos, tokens, gain):
    return pl.pallas_call(
        norm_kernel,
        grid_spec=pltpu.PrefetchScalarGridSpec(
            num_scalar_prefetch=1,
            grid=(1,),
            in_specs=[whole_spec((128, 2048)), whole_spec((1, 2048))],
            out_specs=whole_spec((128, 2048)),
            scratch_shapes=[pltpu.VMEM((128, 2048), BF16)],
        ),
        out_shape=jax.ShapeDtypeStruct((128, 2048), BF16),
        compiler_params=pltpu.CompilerParams(vmem_limit_bytes=VMEM_LIMIT),
        cost_estimate=pl.CostEstimate(flops=10**9, bytes_accessed=2**20, transcendentals=0),
        name="first_norm",
    )(pos, tokens, gain)


def qkv_attention_kernel(pos, *refs):
    pieces, (own_ref, other_ref, o_ref, weight, projected) = refs[:10], refs[10:]
    for zh in range(2):
        for y in range(4):
            at = (zh * 4 + y) * 256
            weight[at : at + 128] = own_ref[pos[y], zh ^ pos[8]]
            weight[at + 128 : at + 256] = other_ref[pos[y], zh ^ pos[8]]

    for part, group in enumerate(((0, 1), (2, 3, 4), (5, 6), (7, 8, 9))):
        rows = jnp.concatenate([pieces[i][...] for i in group], axis=0)
        projected[part * 256 : part * 256 + 256] = jnp.dot(
            rows, weight[...], preferred_element_type=F32
        ).astype(BF16)

    @pl.loop(0, 4)
    def _(i):
        rows = pl.ds(pl.multiple_of(i * 256, 256), 256)
        outs = []
        for head in range(2):
            at = head * 128
            query = projected[rows, at : at + 128]
            key = projected[:, 256 + at : 384 + at]
            value = projected[:, 512 + at : 640 + at]
            scores = lax.dot_general(query, key, (((1,), (1,)), ((), ())), preferred_element_type=F32)
            top = jnp.max(scores, axis=-1, keepdims=True)
            weights = jnp.exp2((scores - top) * (128**-0.5 * 1.4426950408889634))
            total = jnp.sum(weights, axis=-1, keepdims=True)
            mixed = jnp.dot(weights.astype(BF16), value, preferred_element_type=F32)
            outs.append((mixed / total).astype(BF16))
        both = jnp.concatenate(outs, axis=1)
        o_ref[pos[10 + 2 * i]] = both[:128]
        o_ref[pos[11 + 2 * i]] = both[128:]


def qkv_attention(pos, pieces, own, other):
    return pl.pallas_call(
        qkv_attention_kernel,
        grid_spec=pltpu.PrefetchScalarGridSpec(
            num_scalar_prefetch=1,
            grid=(1,),
            in_specs=[whole_spec(piece.shape) for piece in pieces] + [whole_spec((4, 2, 128, 768))] * 2,
            out_specs=whole_spec((8, 128, 256)),
            scratch_shapes=[pltpu.VMEM((2048, 768), BF16), pltpu.VMEM((1024, 768), BF16)],
        ),
        out_shape=jax.ShapeDtypeStruct((8, 128, 256), BF16),
        compiler_params=pltpu.CompilerParams(vmem_limit_bytes=VMEM_LIMIT),
        cost_estimate=pl.CostEstimate(flops=12 * 10**9, bytes_accessed=8 * 2**20, transcendentals=2**21),
        name="qkv_attention",
    )(pos, *pieces, own, other)


def out_kernel(pos, a_ref, *refs):
    own, other = refs[:5], refs[5:10]
    t_ref, g_ref, p_ref, hidden_ref, normed_ref, table_ref, product = refs[10:]
    step = pl.program_id(0)
    heads = jnp.concatenate([a_ref[2 * pos[4 + r] + zl] for r in range(4) for zl in range(2)], axis=1)
    for zh in range(2):
        sides = []
        for held in (own, other):
            blocks = [held[r][2 * zh + zl, 0] for r in range(3) for zl in range(2)]
            blocks += [held[3 + zh][zl, 0] for zl in range(2)]
            sides.append(jnp.concatenate(blocks, axis=0))
        both = jnp.dot(heads, jnp.concatenate(sides, axis=1), preferred_element_type=F32)
        product[zh * 8 + step * 2 + pos[9]] = both[:, :128]
        product[zh * 8 + step * 2 + 1 - pos[9]] = both[:, 128:]

    @pl.when(step == pl.num_programs(0) - 1)
    def _():
        mixed = jnp.concatenate([product[i] for i in range(16)], axis=1)
        hidden = (t_ref[...].astype(F32) + mixed).astype(BF16)
        hidden_ref[...] = hidden
        normed = layer_norm(hidden, g_ref[...]).astype(BF16)
        normed_ref[...] = normed
        slots = lax.broadcasted_iota(jnp.int32, (256, 128), 0)
        placing = jnp.where(slots == p_ref[...], 1.0, 0.0).astype(BF16)
        table = jnp.dot(placing, normed, preferred_element_type=F32).astype(BF16).reshape(64, 4, 2048)
        table_ref[:, 0] = table
        table_ref[:, 1] = table


def out_projection(pos, attended, own, other, tokens, gain, position):
    whole = whole_spec((128, 2048))
    weights = [
        pl.BlockSpec((piece.shape[0], 1, 256, 128), lambda i, p: (0, i, 0, 0)) for piece in (*own, *other)
    ]
    return pl.pallas_call(
        out_kernel,
        grid_spec=pltpu.PrefetchScalarGridSpec(
            num_scalar_prefetch=1,
            grid=(4,),
            in_specs=[
                whole_spec((8, 128, 256)),
                *weights,
                whole,
                whole_spec((1, 2048)),
                whole_spec((1, 128)),
            ],
            out_specs=[whole, whole, whole_spec((64, 2, 4, 2048))],
            scratch_shapes=[pltpu.VMEM((16, 128, 128), F32)],
        ),
        out_shape=[jax.ShapeDtypeStruct((128, 2048), BF16)] * 2 + [jax.ShapeDtypeStruct((64, 2, 4, 2048), BF16)],
        compiler_params=pltpu.CompilerParams(vmem_limit_bytes=VMEM_LIMIT),
        cost_estimate=pl.CostEstimate(flops=6 * 10**9, bytes_accessed=9 * 2**20, transcendentals=0),
        name="out_projection",
    )(pos, attended, *own, *other, tokens, gain, position)


def dense_kernel(*refs):
    pieces, (up_ref, down_ref) = refs[:2], refs[2:4]
    outs, (rows, total) = refs[4:6], refs[6:]
    step = pl.program_id(0)

    @pl.when(step == 0)
    def _():
        for i, piece in enumerate(pieces):
            rows[128 * i : 128 * i + 128] = piece[...]
        total[...] = jnp.zeros_like(total)

    width = up_ref.shape[-1]
    up = up_ref[...].reshape(2048, width)
    inner = gelu(jnp.dot(rows[...], up, preferred_element_type=F32)).astype(BF16)
    down = jnp.concatenate(
        [
            jnp.concatenate([down_ref[r // 8, 0, r % 8, :, at : at + 128] for r in range(16)], axis=1)
            for at in range(0, width, 128)
        ],
        axis=0,
    )
    total[...] += jnp.dot(inner, down, preferred_element_type=F32)

    @pl.when(step == pl.num_programs(0) - 1)
    def _():
        for i, out in enumerate(outs):
            out[...] = total[128 * i : 128 * i + 128].astype(BF16)


def dense_branch(pieces, weights):
    width = 512
    whole = [pl.BlockSpec(piece.shape, lambda j: (0, 0)) for piece in pieces]
    up = pl.BlockSpec((2, 1, 8, 128, width), lambda j: (0, j // 2, 0, 0, j % 2))
    down = pl.BlockSpec((2, 1, 8, 128, width), lambda j: (0, j // 2, 0, 1, j % 2))
    return pl.pallas_call(
        dense_kernel,
        grid=(4,),
        in_specs=whole + [up, down],
        out_specs=whole,
        scratch_shapes=[pltpu.VMEM((256, 2048), BF16), pltpu.VMEM((256, 2048), F32)],
        out_shape=[jax.ShapeDtypeStruct(piece.shape, BF16) for piece in pieces],
        compiler_params=pltpu.CompilerParams(vmem_limit_bytes=VMEM_LIMIT),
        cost_estimate=pl.CostEstimate(flops=7 * 10**9, bytes_accessed=20 * 2**20, transcendentals=2**20),
        name="dense_branch",
    )(*pieces, weights, weights)


def expert_kernel(x_ref, up_ref, down_ref, o_ref, rows, total):
    step = pl.program_id(0)

    @pl.when(step == 0)
    def _():
        rows[...] = x_ref[...].reshape(512, 2048)
        total[...] = jnp.zeros_like(total)

    inner = gelu(jnp.dot(rows[...], up_ref[...], preferred_element_type=F32)).astype(BF16)
    total[...] += jnp.dot(inner, down_ref[...], preferred_element_type=F32)

    @pl.when(step == pl.num_programs(0) - 1)
    def _():
        o_ref[...] = total[...].astype(BF16).reshape(128, 4, 2048)


def expert_branch(rows, up, down):
    width = 512
    whole = pl.BlockSpec((128, 4, 2048), lambda j: (0, 0, 0))
    return pl.pallas_call(
        expert_kernel,
        grid=(2048 // width,),
        in_specs=[
            whole,
            pl.BlockSpec((None, 2048, width), lambda j: (0, 0, j)),
            pl.BlockSpec((None, width, 2048), lambda j: (0, j, 0)),
        ],
        out_specs=whole,
        out_shape=jax.ShapeDtypeStruct((128, 4, 2048), BF16),
        scratch_shapes=[pltpu.VMEM((512, 2048), BF16), pltpu.VMEM((512, 2048), F32)],
        compiler_params=pltpu.CompilerParams(vmem_limit_bytes=VMEM_LIMIT),
        cost_estimate=pl.CostEstimate(flops=12 * 10**9, bytes_accessed=20 * 2**20, transcendentals=2**20),
        name="expert_branch",
    )(rows, up, down)


def final_kernel(h_ref, own_ref, back_ref, ahead_ref, far_ref, r_ref, s_ref, o_ref):
    place = lax.broadcasted_iota(jnp.int32, (128, 512), 1)
    first = s_ref[...]
    picking = jnp.where((place == first) | (place == first + 4), 1.0, 0.0).astype(BF16)
    experts = jnp.dot(picking, r_ref[...].reshape(512, 2048), preferred_element_type=F32)
    dense = own_ref[...].astype(F32) + back_ref[...].astype(F32)
    dense += ahead_ref[...].astype(F32) + far_ref[...].astype(F32)
    o_ref[...] = (h_ref[...].astype(F32) + dense + experts).astype(BF16)


def combined(hidden, dense, returned, first):
    return pl.pallas_call(
        final_kernel,
        out_shape=jax.ShapeDtypeStruct((128, 2048), BF16),
        compiler_params=pltpu.CompilerParams(vmem_limit_bytes=VMEM_LIMIT),
        cost_estimate=pl.CostEstimate(flops=10**9, bytes_accessed=4 * 2**20, transcendentals=0),
        name="combined",
    )(hidden, *dense, returned, first)


def shards(tokens, ln1_gain, qkv_weight, out_weight, ln2_gain, ffn_in, ffn_out, expert_ids, expert_in, expert_out):
    zh, y, c, x, zl = (lax.axis_index(name) for name in ALL)
    ring = [x, lax.rem(x + 3, 4), lax.rem(x + 1, 4), lax.rem(x + 2, 4)]
    rel_rows = [place * 2 + (zl ^ far) for far in range(2) for place in ring]
    pos = jnp.concatenate(
        [ring_slot(jnp.arange(4, dtype=jnp.int32), y), jnp.stack([*ring, zh, c, *rel_rows])]
    ).astype(jnp.int32)

    chosen = expert_ids[:, 0]
    expert_range = jnp.arange(64, dtype=jnp.int32)
    one_hot = (chosen[:, None] == expert_range[None, :]).astype(jnp.int32)
    earlier = jnp.cumsum(one_hot, axis=0) - one_hot
    slot = jnp.sum(earlier * one_hot, axis=1)
    position = (chosen * 4 + slot)[None, :]
    first = (8 * chosen + slot)[:, None]

    down_blocks = ffn_out.reshape(8, 128, 128).transpose(1, 0, 2).reshape(128, 1024)
    packed = jnp.concatenate([ffn_in, down_blocks])
    dense_weights = lax.all_gather(packed, ("zh", "zl", "y", "c")).reshape(2, 2, 8, 256, 1024)

    out_block = copies_of_all(out_weight, ("zh", "zl", "y")).reshape(4, 4, 256, 128)
    normed = first_norm(pos, tokens, ln1_gain[None])
    qkv = qkv_weight.transpose(0, 2, 1, 3).reshape(128, 768)
    qkv = jnp.stack([qkv, swapped(qkv, "zh")])
    qkv = jnp.stack([qkv, *(moved(qkv, "y", step) for step in (1, 3, 2))])
    own, back, ahead, far_low, far_high = ring_parts(normed, "x")
    side = swapped(normed, "zl")
    side_back, side_ahead = moved(side, "x", 1), moved(side, "x", 3)
    side_low, side_high = swapped(far_low, "zl"), swapped(far_high, "zl")
    image = [own, back, ahead, far_low, far_high, side, side_back, side_ahead, side_low, side_high]
    qkv_other = swapped(qkv, "c")

    out_own = ring_parts(out_block, "x")
    out_other = [swapped(piece, "c") for piece in out_own]

    attended = qkv_attention(pos, image, qkv, qkv_other)
    attended = exchanged(attended, ("x", "zl"))
    hidden, normed_two, outgoing = out_projection(pos, attended, out_own, out_other, tokens, ln2_gain[None], position)

    arrived = exchanged(outgoing.reshape(128, 4, 2048), ALL)
    from_back, from_ahead, from_far = (
        moved(normed_two, "x", step) for step in (1, 3, 2)
    )
    halves = expert_branch(arrived, expert_in, expert_out)
    returned = exchanged(halves, ALL)

    to_far, to_ahead = dense_branch((from_far, from_ahead), dense_weights)
    to_back, dense = dense_branch((from_back, normed_two), dense_weights)
    home = [moved(to_far, "x", 2), moved(to_ahead, "x", 1), moved(to_back, "x", 3)]
    return combined(hidden, [dense, *home], returned, first)


def solution(mesh):
    split = Mesh(mesh.devices.reshape(2, 4, 2, 4, 2), ALL)
    row, col = ("zh", "y", "c"), ("x", "zl")
    in_specs = (
        P(ALL, None),
        P(),
        P(row, col, None, None),
        P(col, row),
        P(),
        P(row, col),
        P(col, row),
        P(ALL, None),
        P(ALL, None, None),
        P(ALL, None, None),
    )

    return jax.shard_map(shards, mesh=split, in_specs=in_specs, out_specs=P(ALL, None), check_vma=False)
```

```python
import jax
import jax.numpy as jnp
from jax import lax
from jax.experimental import pallas as pl
from jax.experimental.pallas import tpu as pltpu
from jax.sharding import Mesh
from jax.sharding import PartitionSpec as P


ALL = ("zh", "y", "c", "x", "zl")
BF16 = jnp.bfloat16
F32 = jnp.float32
VMEM_LIMIT = 60 * 2**20


def gelu(value):
    return value * 0.5 * (1.0 + lax.erf(value * (0.5**0.5)))


def moved(array, axis, step):
    return lax.ppermute(array, axis, [(i, (i + step) % 4) for i in range(4)])


def swapped(array, axis):
    return lax.ppermute(array, axis, [(0, 1), (1, 0)])


def exchanged(array, axes):
    return lax.all_to_all(array, axes, 0, 0, tiled=True)


def copies_of_all(array, axes):
    return exchanged(jnp.broadcast_to(array, (lax.axis_size(axes), *array.shape)), axes)


def ring_parts(array, axis):
    half = array.shape[0] // 2
    back, ahead = moved(array, axis, 1), moved(array, axis, 3)
    far_low, far_high = moved(back[:half], axis, 1), moved(ahead[half:], axis, 3)
    return array, back, ahead, far_low, far_high


def ring_slot(index, own):
    away = lax.rem(index - own + 4, 4)
    return jnp.where(away == 0, 0, jnp.where(away == 3, 1, jnp.where(away == 1, 2, 3)))


def layer_norm(rows, gain):
    rows = rows.astype(F32)
    centered = rows - jnp.mean(rows, axis=-1, keepdims=True)
    spread = jnp.mean(centered * centered, axis=-1, keepdims=True)
    return centered * lax.rsqrt(spread + 1e-06) * gain


def core_block(pos, place):
    pair, side = place // 2, place % 2
    return pl.ds(pl.multiple_of((2 * pair + (side ^ pos[9])) * 128, 128), 128)


def whole_spec(shape):
    return pl.BlockSpec(shape, lambda i, p: (0,) * len(shape))


def norm_kernel(pos, x_ref, g_ref, o_ref, rows):
    rows[...] = layer_norm(x_ref[...], g_ref[...]).astype(BF16)
    for place in range(16):
        o_ref[:, place * 128 : place * 128 + 128] = rows[:, core_block(pos, place)]


def first_norm(pos, tokens, gain):
    return pl.pallas_call(
        norm_kernel,
        grid_spec=pltpu.PrefetchScalarGridSpec(
            num_scalar_prefetch=1,
            grid=(1,),
            in_specs=[whole_spec((128, 2048)), whole_spec((1, 2048))],
            out_specs=whole_spec((128, 2048)),
            scratch_shapes=[pltpu.VMEM((128, 2048), BF16)],
        ),
        out_shape=jax.ShapeDtypeStruct((128, 2048), BF16),
        compiler_params=pltpu.CompilerParams(vmem_limit_bytes=VMEM_LIMIT),
        cost_estimate=pl.CostEstimate(flops=10**9, bytes_accessed=2**20, transcendentals=0),
        name="first_norm",
    )(pos, tokens, gain)


def qkv_attention_kernel(pos, *refs):
    pieces, (own_ref, other_ref, o_ref, weight, projected) = refs[:10], refs[10:]
    for zh in range(2):
        for y in range(4):
            at = (zh * 4 + y) * 256
            weight[at : at + 128] = own_ref[pos[y], zh ^ pos[8]]
            weight[at + 128 : at + 256] = other_ref[pos[y], zh ^ pos[8]]

    for part, group in enumerate(((0, 1), (2, 3, 4), (5, 6), (7, 8, 9))):
        rows = jnp.concatenate([pieces[i][...] for i in group], axis=0)
        projected[part * 256 : part * 256 + 256] = jnp.dot(
            rows, weight[...], preferred_element_type=F32
        ).astype(BF16)

    @pl.loop(0, 4)
    def _(i):
        rows = pl.ds(pl.multiple_of(i * 256, 256), 256)
        outs = []
        for head in range(2):
            at = head * 128
            query = projected[rows, at : at + 128]
            key = projected[:, 256 + at : 384 + at]
            value = projected[:, 512 + at : 640 + at]
            scores = lax.dot_general(query, key, (((1,), (1,)), ((), ())), preferred_element_type=F32)
            top = jnp.max(scores, axis=-1, keepdims=True)
            weights = jnp.exp2((scores - top) * (128**-0.5 * 1.4426950408889634))
            total = jnp.sum(weights, axis=-1, keepdims=True)
            mixed = jnp.dot(weights.astype(BF16), value, preferred_element_type=F32)
            outs.append((mixed / total).astype(BF16))
        both = jnp.concatenate(outs, axis=1)
        o_ref[pos[10 + 2 * i]] = both[:128]
        o_ref[pos[11 + 2 * i]] = both[128:]


def qkv_attention(pos, pieces, own, other):
    return pl.pallas_call(
        qkv_attention_kernel,
        grid_spec=pltpu.PrefetchScalarGridSpec(
            num_scalar_prefetch=1,
            grid=(1,),
            in_specs=[whole_spec(piece.shape) for piece in pieces] + [whole_spec((4, 2, 128, 768))] * 2,
            out_specs=whole_spec((8, 128, 256)),
            scratch_shapes=[pltpu.VMEM((2048, 768), BF16), pltpu.VMEM((1024, 768), BF16)],
        ),
        out_shape=jax.ShapeDtypeStruct((8, 128, 256), BF16),
        compiler_params=pltpu.CompilerParams(vmem_limit_bytes=VMEM_LIMIT),
        cost_estimate=pl.CostEstimate(flops=12 * 10**9, bytes_accessed=8 * 2**20, transcendentals=2**21),
        name="qkv_attention",
    )(pos, *pieces, own, other)


def out_kernel(pos, a_ref, *refs):
    own, other = refs[:5], refs[5:10]
    t_ref, g_ref, p_ref, hidden_ref, normed_ref, table_ref, product = refs[10:]
    step = pl.program_id(0)
    heads = jnp.concatenate([a_ref[2 * pos[4 + r] + zl] for r in range(4) for zl in range(2)], axis=1)
    for zh in range(2):
        sides = []
        for held in (own, other):
            blocks = [held[r][2 * zh + zl, 0] for r in range(3) for zl in range(2)]
            blocks += [held[3 + zh][zl, 0] for zl in range(2)]
            sides.append(jnp.concatenate(blocks, axis=0))
        both = jnp.dot(heads, jnp.concatenate(sides, axis=1), preferred_element_type=F32)
        product[zh * 8 + step * 2 + pos[9]] = both[:, :128]
        product[zh * 8 + step * 2 + 1 - pos[9]] = both[:, 128:]

    @pl.when(step == pl.num_programs(0) - 1)
    def _():
        mixed = jnp.concatenate([product[i] for i in range(16)], axis=1)
        hidden = (t_ref[...].astype(F32) + mixed).astype(BF16)
        hidden_ref[...] = hidden
        normed = layer_norm(hidden, g_ref[...]).astype(BF16)
        normed_ref[...] = normed
        slots = lax.broadcasted_iota(jnp.int32, (256, 128), 0)
        placing = jnp.where(slots == p_ref[...], 1.0, 0.0).astype(BF16)
        table = jnp.dot(placing, normed, preferred_element_type=F32).astype(BF16).reshape(64, 4, 2048)
        table_ref[:, 0] = table
        table_ref[:, 1] = table


def out_projection(pos, attended, own, other, tokens, gain, position):
    whole = whole_spec((128, 2048))
    weights = [
        pl.BlockSpec((piece.shape[0], 1, 256, 128), lambda i, p: (0, i, 0, 0)) for piece in (*own, *other)
    ]
    return pl.pallas_call(
        out_kernel,
        grid_spec=pltpu.PrefetchScalarGridSpec(
            num_scalar_prefetch=1,
            grid=(4,),
            in_specs=[
                whole_spec((8, 128, 256)),
                *weights,
                whole,
                whole_spec((1, 2048)),
                whole_spec((1, 128)),
            ],
            out_specs=[whole, whole, whole_spec((64, 2, 4, 2048))],
            scratch_shapes=[pltpu.VMEM((16, 128, 128), F32)],
        ),
        out_shape=[jax.ShapeDtypeStruct((128, 2048), BF16)] * 2 + [jax.ShapeDtypeStruct((64, 2, 4, 2048), BF16)],
        compiler_params=pltpu.CompilerParams(vmem_limit_bytes=VMEM_LIMIT),
        cost_estimate=pl.CostEstimate(flops=6 * 10**9, bytes_accessed=9 * 2**20, transcendentals=0),
        name="out_projection",
    )(pos, attended, *own, *other, tokens, gain, position)


def dense_kernel(*refs):
    pieces, (up_ref, down_ref) = refs[:4], refs[4:6]
    outs, (rows, total) = refs[6:10], refs[10:]
    step = pl.program_id(0)

    @pl.when(step == 0)
    def _():
        for i, piece in enumerate(pieces):
            rows[128 * i : 128 * i + 128] = piece[...]
        total[...] = jnp.zeros_like(total)

    width = up_ref.shape[-1]
    up = up_ref[...].reshape(2048, width)
    inner = gelu(jnp.dot(rows[...], up, preferred_element_type=F32)).astype(BF16)
    down = jnp.concatenate(
        [
            jnp.concatenate([down_ref[r // 8, 0, r % 8, :, at : at + 128] for r in range(16)], axis=1)
            for at in range(0, width, 128)
        ],
        axis=0,
    )
    total[...] += jnp.dot(inner, down, preferred_element_type=F32)

    @pl.when(step == pl.num_programs(0) - 1)
    def _():
        for i, out in enumerate(outs):
            out[...] = total[128 * i : 128 * i + 128].astype(BF16)


def dense_branch(pieces, weights):
    width = 512
    whole = [pl.BlockSpec(piece.shape, lambda j: (0, 0)) for piece in pieces]
    up = pl.BlockSpec((2, 1, 8, 128, width), lambda j: (0, j // 2, 0, 0, j % 2))
    down = pl.BlockSpec((2, 1, 8, 128, width), lambda j: (0, j // 2, 0, 1, j % 2))
    return pl.pallas_call(
        dense_kernel,
        grid=(4,),
        in_specs=whole + [up, down],
        out_specs=whole,
        scratch_shapes=[pltpu.VMEM((512, 2048), BF16), pltpu.VMEM((512, 2048), F32)],
        out_shape=[jax.ShapeDtypeStruct(piece.shape, BF16) for piece in pieces],
        compiler_params=pltpu.CompilerParams(vmem_limit_bytes=VMEM_LIMIT),
        cost_estimate=pl.CostEstimate(flops=14 * 10**9, bytes_accessed=20 * 2**20, transcendentals=2**20),
        name="dense_branch",
    )(*pieces, weights, weights)


def expert_kernel(x_ref, up_ref, down_ref, o_ref, rows, total):
    step = pl.program_id(0)

    @pl.when(step == 0)
    def _():
        rows[...] = x_ref[...].reshape(512, 2048)
        total[...] = jnp.zeros_like(total)

    inner = gelu(jnp.dot(rows[...], up_ref[...], preferred_element_type=F32)).astype(BF16)
    total[...] += jnp.dot(inner, down_ref[...], preferred_element_type=F32)

    @pl.when(step == pl.num_programs(0) - 1)
    def _():
        o_ref[...] = total[...].astype(BF16).reshape(128, 4, 2048)


def expert_branch(rows, up, down):
    width = 512
    whole = pl.BlockSpec((128, 4, 2048), lambda j: (0, 0, 0))
    return pl.pallas_call(
        expert_kernel,
        grid=(2048 // width,),
        in_specs=[
            whole,
            pl.BlockSpec((None, 2048, width), lambda j: (0, 0, j)),
            pl.BlockSpec((None, width, 2048), lambda j: (0, j, 0)),
        ],
        out_specs=whole,
        out_shape=jax.ShapeDtypeStruct((128, 4, 2048), BF16),
        scratch_shapes=[pltpu.VMEM((512, 2048), BF16), pltpu.VMEM((512, 2048), F32)],
        compiler_params=pltpu.CompilerParams(vmem_limit_bytes=VMEM_LIMIT),
        cost_estimate=pl.CostEstimate(flops=12 * 10**9, bytes_accessed=20 * 2**20, transcendentals=2**20),
        name="expert_branch",
    )(rows, up, down)


def final_kernel(h_ref, own_ref, back_ref, ahead_ref, far_ref, r_ref, s_ref, o_ref):
    place = lax.broadcasted_iota(jnp.int32, (128, 512), 1)
    first = s_ref[...]
    picking = jnp.where((place == first) | (place == first + 4), 1.0, 0.0).astype(BF16)
    experts = jnp.dot(picking, r_ref[...].reshape(512, 2048), preferred_element_type=F32)
    dense = own_ref[...].astype(F32) + back_ref[...].astype(F32)
    dense += ahead_ref[...].astype(F32) + far_ref[...].astype(F32)
    o_ref[...] = (h_ref[...].astype(F32) + dense + experts).astype(BF16)


def combined(hidden, dense, returned, first):
    return pl.pallas_call(
        final_kernel,
        out_shape=jax.ShapeDtypeStruct((128, 2048), BF16),
        compiler_params=pltpu.CompilerParams(vmem_limit_bytes=VMEM_LIMIT),
        cost_estimate=pl.CostEstimate(flops=10**9, bytes_accessed=4 * 2**20, transcendentals=0),
        name="combined",
    )(hidden, *dense, returned, first)


def shards(tokens, ln1_gain, qkv_weight, out_weight, ln2_gain, ffn_in, ffn_out, expert_ids, expert_in, expert_out):
    zh, y, c, x, zl = (lax.axis_index(name) for name in ALL)
    ring = [x, lax.rem(x + 3, 4), lax.rem(x + 1, 4), lax.rem(x + 2, 4)]
    rel_rows = [place * 2 + (zl ^ far) for far in range(2) for place in ring]
    pos = jnp.concatenate(
        [ring_slot(jnp.arange(4, dtype=jnp.int32), y), jnp.stack([*ring, zh, c, *rel_rows])]
    ).astype(jnp.int32)

    chosen = expert_ids[:, 0]
    expert_range = jnp.arange(64, dtype=jnp.int32)
    one_hot = (chosen[:, None] == expert_range[None, :]).astype(jnp.int32)
    earlier = jnp.cumsum(one_hot, axis=0) - one_hot
    slot = jnp.sum(earlier * one_hot, axis=1)
    position = (chosen * 4 + slot)[None, :]
    first = (8 * chosen + slot)[:, None]

    down_blocks = ffn_out.reshape(8, 128, 128).transpose(1, 0, 2).reshape(128, 1024)
    packed = jnp.concatenate([ffn_in, down_blocks])
    dense_weights = lax.all_gather(packed, ("zh", "zl", "y", "c")).reshape(2, 2, 8, 256, 1024)

    out_block = copies_of_all(out_weight, ("zh", "zl", "y")).reshape(4, 4, 256, 128)
    normed = first_norm(pos, tokens, ln1_gain[None])
    qkv = qkv_weight.transpose(0, 2, 1, 3).reshape(128, 768)
    qkv = jnp.stack([qkv, swapped(qkv, "zh")])
    qkv_own, qkv_back, qkv_ahead, *qkv_far = ring_parts(qkv, "y")
    qkv = jnp.stack([qkv_own, qkv_back, qkv_ahead, jnp.concatenate(qkv_far)])
    own, back, ahead, far_low, far_high = ring_parts(normed, "x")
    side = swapped(normed, "zl")
    side_back, side_ahead = moved(side, "x", 1), moved(side, "x", 3)
    side_low, side_high = swapped(far_low, "zl"), swapped(far_high, "zl")
    image = [own, back, ahead, far_low, far_high, side, side_back, side_ahead, side_low, side_high]
    qkv_other = swapped(qkv, "c")

    out_own = ring_parts(out_block, "x")
    out_other = [swapped(piece, "c") for piece in out_own]

    attended = qkv_attention(pos, image, qkv, qkv_other)
    attended = exchanged(attended, ("x", "zl"))
    hidden, normed_two, outgoing = out_projection(pos, attended, out_own, out_other, tokens, ln2_gain[None], position)

    arrived = exchanged(outgoing.reshape(128, 4, 2048), ALL)
    from_back, from_ahead, from_far = (
        moved(normed_two, "x", step) for step in (1, 3, 2)
    )
    halves = expert_branch(arrived, expert_in, expert_out)
    returned = exchanged(halves, ALL)

    to_far, to_ahead, to_back, dense = dense_branch(
        (from_far, from_ahead, from_back, normed_two), dense_weights
    )
    home = [moved(to_far, "x", 2), moved(to_ahead, "x", 1), moved(to_back, "x", 3)]
    return combined(hidden, [dense, *home], returned, first)


def solution(mesh):
    split = Mesh(mesh.devices.reshape(2, 4, 2, 4, 2), ALL)
    row, col = ("zh", "y", "c"), ("x", "zl")
    in_specs = (
        P(ALL, None),
        P(),
        P(row, col, None, None),
        P(col, row),
        P(),
        P(row, col),
        P(col, row),
        P(ALL, None),
        P(ALL, None, None),
        P(ALL, None, None),
    )

    return jax.shard_map(shards, mesh=split, in_specs=in_specs, out_specs=P(ALL, None), check_vma=False)
```
